32 devices in a mesh: section: 8 (over y, x, core), tp: 4 (over z).
Axes of the slice: x: 2, y: 2, z: 4, core: 2. Of those that a mesh axis runs over, the one named last changes fastest.
Arguments:
- tokens: bfloat16 [512, 2048], P('tp'), may hold values from -6 to 6
- cotangent: bfloat16 [512, 2048], P('tp'), may hold values from -0.119628906 to 0.119628906
- value_weight: bfloat16 [8, 2048, 512], P('section', None, 'tp'), may hold values from -0.125 to 0.125
- output_weight: bfloat16 [8, 2048, 512], P('section', None, 'tp'), may hold values from -0.25 to 0.25
- value_first: float32 [8, 2048, 512], P('section', None, 'tp'), may hold values from -1.8 to 1.8
- output_first: float32 [8, 2048, 512], P('section', None, 'tp'), may hold values from -1.8 to 1.8
- value_second: float32 [8, 2048, 512], P('section', None, 'tp'), may hold values from 0.01 to 1
- output_second: float32 [8, 2048, 512], P('section', None, 'tp'), may hold values from 0.01 to 1
- layer_map: int32 [6], replicated, may hold values from 0 to 3, as said below
- old_section: int32 [4], replicated, may hold values from 0 to 7, as said below
- new_section: int32 [6], replicated, may hold values from 0 to 7, as said below
Outputs:
- new_value_weight: bfloat16 [8, 2048, 512], P('section', None, 'tp')
- new_output_weight: bfloat16 [8, 2048, 512], P('section', None, 'tp')
- new_value_first: float32 [8, 2048, 512], P('section', None, 'tp')
- new_output_first: float32 [8, 2048, 512], P('section', None, 'tp')
- new_value_second: float32 [8, 2048, 512], P('section', None, 'tp')
- new_output_second: float32 [8, 2048, 512], P('section', None, 'tp')
The draws below stay inside these ranges and needn't reach their ends.
Inputs may be any that keep to these rules, and one draw needn't show every extreme that they name: `layer_map`: Non-decreasing; every old layer appears once or twice. `old_section`: strictly increasing. `new_section`: strictly increasing.
All inputs are finite; a program needn't handle non-finite values.
Results may differ from the reference program's by a relative error of at most 0.025.
Values may be sent and summed in bfloat16 or wider, within the bound.
No kernel may reach another device: no remote copies, remote signals or barrier semaphores. Data moves between devices by JAX's collectives and lax.ppermute only.
A program may use at most 128 MiB of HBM per device.

```python
import math
import jax
import jax.numpy as jnp
from jax import lax

D = 2048
KVW = 512
TOKENS = 512
SECTIONS = 8
OLD = 4
NEW = 6


def draw_layer_map(key, part):
    shuffled = jax.random.permutation(jax.random.fold_in(key, 5), OLD)
    doubled = (shuffled < NEW - OLD).astype(jnp.int32)
    bounds = jnp.cumsum(1 + doubled)
    positions = lax.iota(jnp.int32, NEW)
    return jnp.sum((bounds[None, :] <= positions[:, None]).astype(jnp.int32), axis=1).astype(jnp.int32)


def ends_included(key, count):
    shuffled = jax.random.permutation(key, SECTIONS - 2) + 1
    inner = shuffled[:count - 2].astype(jnp.int32)
    first = jnp.zeros((1,), jnp.int32)
    final = jnp.full((1,), SECTIONS - 1, jnp.int32)
    return jnp.sort(jnp.concatenate([first, inner, final])).astype(jnp.int32)


def draw_old_section(key, part):
    return ends_included(jax.random.fold_in(key, 11), OLD)


def draw_new_section(key, part):
    return ends_included(jax.random.fold_in(key, 23), NEW)


def level_of(key, extent, pieces, least, high):
    gain, own = 1.0, jax.random.fold_in(key, 6)
    for dim, shards_of in pieces:
        heights = jnp.exp(jax.random.uniform(jax.random.fold_in(own, dim), (shards_of,), jnp.float32, least / len(pieces), high / len(pieces)))
        gain = gain * jnp.repeat(heights, extent[dim] // shards_of).reshape([-1 if axis == dim else 1 for axis in range(len(extent))])
    return gain


def noise(stream_key, dims, deviation, most, split=(), held_as=jnp.bfloat16):
    entries = deviation * jax.random.normal(stream_key, dims, jnp.float32)
    if split:
        entries = entries * level_of(stream_key, dims, split, -0.22, 0.18)
    return jnp.clip(entries, -most, most).astype(held_as)


def setup_inputs(seed: int = 0) -> dict:
    key_of = jax.random.split(jax.random.key(seed), 12)
    tokens = noise(key_of[0], (TOKENS, D), 1.0, 6.0, ((0, 4),))
    cotangent = noise(key_of[1], (TOKENS, D), 0.02, 0.119628906, ((0, 4),))
    value_weight = noise(key_of[2], (SECTIONS, D, KVW), D ** -0.5, 0.125, ((0, 8), (2, 4)))
    output_weight = noise(key_of[3], (SECTIONS, D, KVW), KVW ** -0.5, 0.25, ((0, 8), (2, 4)))
    value_first = noise(key_of[4], (SECTIONS, D, KVW), 0.3, 1.8, ((0, 8), (2, 4)), jnp.float32)
    output_first = noise(key_of[5], (SECTIONS, D, KVW), 0.3, 1.8, ((0, 8), (2, 4)), jnp.float32)
    value_second = jnp.clip(jnp.exp(math.log(1.0) - 4.6051702 * jax.random.uniform(key_of[6], (SECTIONS, D, KVW), jnp.float32) ** level_of(key_of[6], (SECTIONS, D, KVW), ((0, 8), (2, 4)), -0.2, 0.2)), 0.01, 1.0)
    output_second = jnp.clip(jnp.exp(math.log(1.0) - 4.6051702 * jax.random.uniform(key_of[7], (SECTIONS, D, KVW), jnp.float32) ** level_of(key_of[7], (SECTIONS, D, KVW), ((0, 8), (2, 4)), -0.2, 0.2)), 0.01, 1.0)
    layer_map = draw_layer_map(jax.random.fold_in(key_of[11], 71), 0)
    old_section = draw_old_section(jax.random.fold_in(key_of[11], 71), 0)
    new_section = draw_new_section(jax.random.fold_in(key_of[11], 71), 0)
    return dict(tokens=tokens, cotangent=cotangent, value_weight=value_weight, output_weight=output_weight, value_first=value_first, output_first=output_first, value_second=value_second, output_second=output_second, layer_map=layer_map, old_section=old_section, new_section=new_section)


epsilon = 1e-05
beta_one = 0.9
beta_two = 0.95
step_rate = 0.003
adam_floor = 1e-08

def normalize(stream):
    widened = stream.astype(jnp.float32)
    factor = lax.rsqrt(lax.optimization_barrier(jnp.mean(widened * widened, axis=-1, keepdims=True)) + epsilon)
    return (widened * factor, factor)

def forward_layer(stream, value_full, output_full):
    normed, factor = normalize(stream)
    hidden = normed.astype(jnp.bfloat16)
    preact = jnp.dot(hidden, value_full, preferred_element_type=jnp.float32)
    unit_values = jax.nn.silu(preact).astype(jnp.bfloat16)
    mixing = lax.dot_general(unit_values, output_full, (((1,), (1,)), ((), ())), preferred_element_type=jnp.float32)
    return ((stream.astype(jnp.float32) + mixing).astype(jnp.bfloat16), preact, unit_values)

def backward_layer(stream, preact, grad_out, value_full, output_full):
    grad_units = jnp.dot(grad_out, output_full, preferred_element_type=jnp.float32)
    gate_value = jax.nn.sigmoid(preact)
    grad_inner = (grad_units * gate_value * (1.0 + preact * (1.0 - gate_value))).astype(jnp.bfloat16)
    grad_hidden = lax.dot_general(grad_inner, value_full, (((1,), (1,)), ((), ())), preferred_element_type=jnp.float32)
    normed, factor = normalize(stream)
    grad_stream = factor * (grad_hidden - normed * lax.optimization_barrier(jnp.mean(grad_hidden * normed, axis=-1, keepdims=True)))
    return ((grad_out.astype(jnp.float32) + grad_stream).astype(jnp.bfloat16), grad_inner)

def adam_update(weight, first, second, gradient):
    first_new = beta_one * first + (1.0 - beta_one) * gradient
    second_new = beta_two * second + (1.0 - beta_two) * gradient * gradient
    weight_new = (weight.astype(jnp.float32) - step_rate * first_new / (jnp.sqrt(second_new) + adam_floor)).astype(jnp.bfloat16)
    return (weight_new, first_new, second_new)

def reference(tokens, cotangent, value_weight, output_weight, value_first, output_first, value_second, output_second, layer_map, old_section, new_section):
    layer_count = layer_map.shape[0]
    sources = []
    saved_layers = []
    stream = tokens
    for layer_index in range(layer_count):
        source = old_section[layer_map[layer_index]]
        sources.append(source)
        result, preact, unit_values = forward_layer(stream, value_weight[source], output_weight[source])
        saved_layers.append((stream, preact, unit_values))
        stream = result
    flowing = cotangent
    outputs = [jnp.zeros(value_weight.shape, jnp.bfloat16), jnp.zeros(value_weight.shape, jnp.bfloat16), jnp.zeros(value_weight.shape, jnp.float32), jnp.zeros(value_weight.shape, jnp.float32), jnp.zeros(value_weight.shape, jnp.float32), jnp.zeros(value_weight.shape, jnp.float32)]
    for layer_index in reversed(range(layer_count)):
        source = sources[layer_index]
        stream_in, preact, unit_values = saved_layers[layer_index]
        result, grad_inner = backward_layer(stream_in, preact, flowing, value_weight[source], output_weight[source])
        hidden = normalize(stream_in)[0].astype(jnp.bfloat16)
        grad_value = lax.dot_general(hidden, grad_inner, (((0,), (0,)), ((), ())), preferred_element_type=jnp.float32)
        grad_output = lax.dot_general(flowing, unit_values, (((0,), (0,)), ((), ())), preferred_element_type=jnp.float32)
        value_new = adam_update(value_weight[source], value_first[source], value_second[source], grad_value)
        output_new = adam_update(output_weight[source], output_first[source], output_second[source], grad_output)
        target = new_section[layer_index]
        outputs[0] = outputs[0].at[target].set(value_new[0])
        outputs[1] = outputs[1].at[target].set(output_new[0])
        outputs[2] = outputs[2].at[target].set(value_new[1])
        outputs[3] = outputs[3].at[target].set(output_new[1])
        outputs[4] = outputs[4].at[target].set(value_new[2])
        outputs[5] = outputs[5].at[target].set(output_new[2])
        flowing = result
    return (outputs[0], outputs[1], outputs[2], outputs[3], outputs[4], outputs[5])
```

```python
import functools

import jax
import jax.numpy as jnp
from jax import lax
from jax.experimental import pallas as pl
from jax.experimental.pallas import tpu as pltpu
from jax.sharding import PartitionSpec as P

epsilon = 1e-05
beta_one = 0.9
beta_two = 0.95
step_rate = 0.003
adam_floor = 1e-08


def passed_along(block, axis, distance):
    devices = range(lax.axis_size(axis))
    route = [(i - distance, i) for i in devices if i - distance in devices]
    return lax.ppermute(block, axis, route)


def normalize(stream):
    widened = stream.astype(jnp.float32)
    factor = lax.rsqrt(jnp.mean(widened * widened, axis=-1, keepdims=True) + epsilon)
    return (widened * factor, factor)


def forward_layer(stream, value_full, output_full):
    normed, factor = normalize(stream)
    hidden = normed.astype(jnp.bfloat16)
    preact = jnp.dot(hidden, value_full, preferred_element_type=jnp.float32)
    unit_values = jax.nn.silu(preact).astype(jnp.bfloat16)
    mixing = lax.dot_general(
        unit_values, output_full, (((1,), (1,)), ((), ())), preferred_element_type=jnp.float32
    )
    return ((stream.astype(jnp.float32) + mixing).astype(jnp.bfloat16), preact, unit_values)


def backward_layer(stream, preact, grad_out, value_full, output_full):
    grad_units = jnp.dot(grad_out, output_full, preferred_element_type=jnp.float32)
    gate_value = jax.nn.sigmoid(preact)
    grad_inner = (grad_units * gate_value * (1.0 + preact * (1.0 - gate_value))).astype(
        jnp.bfloat16
    )
    grad_hidden = lax.dot_general(
        grad_inner, value_full, (((1,), (1,)), ((), ())), preferred_element_type=jnp.float32
    )
    normed, factor = normalize(stream)
    grad_stream = factor * (
        grad_hidden - normed * jnp.mean(grad_hidden * normed, axis=-1, keepdims=True)
    )
    return ((grad_out.astype(jnp.float32) + grad_stream).astype(jnp.bfloat16), grad_inner)


def hand_over(values, offset):
    return passed_along(values, "section", offset)


def adam_update(weight, first, second, gradient):
    first_new = beta_one * first + (1.0 - beta_one) * gradient
    second_new = beta_two * second + (1.0 - beta_two) * gradient * gradient
    weight_new = (
        weight.astype(jnp.float32) - step_rate * first_new / (jnp.sqrt(second_new) + adam_floor)
    ).astype(jnp.bfloat16)
    return (weight_new[None], first_new[None], second_new[None])


def cascade_body(
    tokens,
    cotangent,
    value_weight,
    output_weight,
    value_first,
    output_first,
    value_second,
    output_second,
    layer_map,
    old_section,
    new_section,
):
    sections = lax.axis_size("section")
    myself = lax.axis_index("section")
    positions = lax.iota(jnp.int32, sections)
    owner_match = new_section[None, :] == positions[:, None]
    has_layer = jnp.any(owner_match, axis=1)
    new_index = jnp.sum(
        jnp.where(owner_match, lax.iota(jnp.int32, new_section.shape[0])[None, :], 0), axis=1
    )
    map_match = new_index[:, None] == lax.iota(jnp.int32, layer_map.shape[0])[None, :]
    old_index = jnp.sum(jnp.where(map_match, layer_map[None, :], 0), axis=1)
    section_match = old_index[:, None] == lax.iota(jnp.int32, old_section.shape[0])[None, :]
    source = jnp.sum(jnp.where(section_match, old_section[None, :], 0), axis=1)
    holds_layer = jnp.any((positions == myself) & has_layer)
    keep_mask = has_layer.astype(jnp.float32)[:, None, None]
    spread_pieces = (
        lax.all_to_all(
            value_weight.astype(jnp.float32), "section", split_axis=1, concat_axis=0, tiled=True
        ),
        lax.all_to_all(
            output_weight.astype(jnp.float32), "section", split_axis=1, concat_axis=0, tiled=True
        ),
        lax.all_to_all(value_first, "section", split_axis=1, concat_axis=0, tiled=True),
        lax.all_to_all(output_first, "section", split_axis=1, concat_axis=0, tiled=True),
        lax.all_to_all(value_second, "section", split_axis=1, concat_axis=0, tiled=True),
        lax.all_to_all(output_second, "section", split_axis=1, concat_axis=0, tiled=True),
    )
    chosen = [jnp.take(portion, source, axis=0) * keep_mask for portion in spread_pieces]
    arrived = (
        lax.all_to_all(chosen[0], "section", split_axis=0, concat_axis=1, tiled=True),
        lax.all_to_all(chosen[1], "section", split_axis=0, concat_axis=1, tiled=True),
        lax.all_to_all(chosen[2], "section", split_axis=0, concat_axis=1, tiled=True),
        lax.all_to_all(chosen[3], "section", split_axis=0, concat_axis=1, tiled=True),
        lax.all_to_all(chosen[4], "section", split_axis=0, concat_axis=1, tiled=True),
        lax.all_to_all(chosen[5], "section", split_axis=0, concat_axis=1, tiled=True),
    )
    value_local = arrived[0][0].astype(jnp.bfloat16)
    output_local = arrived[1][0].astype(jnp.bfloat16)
    first_value = arrived[2][0]
    first_output = arrived[3][0]
    second_value = arrived[4][0]
    second_output = arrived[5][0]
    value_full, output_full = (
        lax.all_gather(value_local, "tp", axis=1, tiled=True),
        lax.all_gather(output_local, "tp", axis=1, tiled=True),
    )
    row_count, feature_count = tokens.shape
    channel_count = value_full.shape[1]
    blocks = 1
    block_rows = row_count // blocks
    step_count = sections + blocks - 1
    token_blocks = tokens.reshape(blocks, block_rows, feature_count)
    grad_blocks = cotangent.reshape(blocks, block_rows, feature_count)

    def forward_step(step_index, loop_state):
        stream, saved_in, saved_pre, saved_units = loop_state
        entering = token_blocks[jnp.minimum(step_index, blocks - 1)]
        stream = jnp.where(myself == 0, entering, stream)
        block_slot = step_index - myself
        active = (block_slot >= 0) & (block_slot < blocks)
        block_place = jnp.clip(block_slot, 0, blocks - 1)
        result, preact, unit_values = forward_layer(stream, value_full, output_full)
        result = jnp.where(holds_layer, result, stream)
        saved_in = jnp.where(
            active, lax.dynamic_update_index_in_dim(saved_in, stream, block_place, 0), saved_in
        )
        saved_pre = jnp.where(
            active, lax.dynamic_update_index_in_dim(saved_pre, preact, block_place, 0), saved_pre
        )
        saved_units = jnp.where(
            active,
            lax.dynamic_update_index_in_dim(saved_units, unit_values, block_place, 0),
            saved_units,
        )
        return (hand_over(result, 1), saved_in, saved_pre, saved_units)

    forward_init = (
        token_blocks[0],
        jnp.zeros((blocks, block_rows, feature_count), jnp.bfloat16),
        jnp.zeros((blocks, block_rows, channel_count), jnp.float32),
        jnp.zeros((blocks, block_rows, channel_count), jnp.bfloat16),
    )
    stream_last, saved_in, saved_pre, saved_units = lax.fori_loop(
        0, step_count, forward_step, forward_init
    )

    def backward_step(step_index, loop_state):
        flowing, saved_grad, saved_inner = loop_state
        entering = grad_blocks[jnp.minimum(step_index, blocks - 1)]
        flowing = jnp.where(myself == sections - 1, entering, flowing)
        block_slot = step_index - (sections - 1 - myself)
        active = (block_slot >= 0) & (block_slot < blocks)
        block_place = jnp.clip(block_slot, 0, blocks - 1)
        stream_in = saved_in[block_place]
        preact = saved_pre[block_place]
        result, grad_inner = backward_layer(stream_in, preact, flowing, value_full, output_full)
        result = jnp.where(holds_layer, result, flowing)
        saved_grad = jnp.where(
            active, lax.dynamic_update_index_in_dim(saved_grad, flowing, block_place, 0), saved_grad
        )
        saved_inner = jnp.where(
            active,
            lax.dynamic_update_index_in_dim(saved_inner, grad_inner, block_place, 0),
            saved_inner,
        )
        return (hand_over(result, -1), saved_grad, saved_inner)

    backward_init = (
        grad_blocks[0],
        jnp.zeros((blocks, block_rows, feature_count), jnp.bfloat16),
        jnp.zeros((blocks, block_rows, channel_count), jnp.bfloat16),
    )
    flowing_last, saved_grad, saved_inner = lax.fori_loop(
        0, step_count, backward_step, backward_init
    )
    hidden_all = normalize(saved_in.reshape(row_count, feature_count))[0].astype(jnp.bfloat16)
    grad_value = lax.dot_general(
        hidden_all,
        saved_inner.reshape(row_count, channel_count),
        (((0,), (0,)), ((), ())),
        preferred_element_type=jnp.float32,
    )
    grad_output = lax.dot_general(
        saved_grad.reshape(row_count, feature_count),
        saved_units.reshape(row_count, channel_count),
        (((0,), (0,)), ((), ())),
        preferred_element_type=jnp.float32,
    )
    grad_value, grad_output = (
        lax.psum_scatter(
            grad_value.astype(jnp.bfloat16), "tp", scatter_dimension=1, tiled=True
        ).astype(jnp.float32),
        lax.psum_scatter(
            grad_output.astype(jnp.bfloat16), "tp", scatter_dimension=1, tiled=True
        ).astype(jnp.float32),
    )
    owned = holds_layer.astype(jnp.float32)
    grad_value = grad_value * owned
    grad_output = grad_output * owned
    value_new = adam_update(value_local, first_value, second_value, grad_value)
    output_new = adam_update(output_local, first_output, second_output, grad_output)
    return (value_new[0], output_new[0], value_new[1], output_new[1], value_new[2], output_new[2])


vmem_budget = 58 * 2**20


def layer_tables(layer_map, old_section, new_section, sections):
    positions = lax.iota(jnp.int32, sections)
    owner_match = new_section[None, :] == positions[:, None]
    has_layer = jnp.any(owner_match, axis=1)
    new_index = jnp.sum(
        jnp.where(owner_match, lax.iota(jnp.int32, new_section.shape[0])[None, :], 0), axis=1
    )
    map_match = new_index[:, None] == lax.iota(jnp.int32, layer_map.shape[0])[None, :]
    old_index = jnp.sum(jnp.where(map_match, layer_map[None, :], 0), axis=1)
    section_match = old_index[:, None] == lax.iota(jnp.int32, old_section.shape[0])[None, :]
    source = jnp.sum(jnp.where(section_match, old_section[None, :], 0), axis=1)
    return (has_layer, jnp.where(has_layer, new_index, -1), source)


def exchanged(block, mask):
    sections = lax.axis_size("section")
    return lax.ppermute(block, "section", [(i, i ^ mask) for i in range(sections)])


def rotated(block, distance):
    count = lax.axis_size("tp")
    return lax.ppermute(block, "tp", [(i, (i + distance) % count) for i in range(count)])


def token_share(block):
    sections, count = lax.axis_size("section"), lax.axis_size("tp")
    share = count // 2
    parts = []
    for slot in range(share):
        route = [
            (s * count + z, s * count + (z + slot + (s % 2) * share) % count)
            for s in range(sections)
            for z in range(count)
        ]
        parts.append(lax.ppermute(block, ("section", "tp"), route))
    return jnp.concatenate(parts, axis=0)


def gathered_pieces(block):
    sections, count = lax.axis_size("section"), lax.axis_size("tp")
    column = jnp.stack([block] + [rotated(block, r) for r in range(1, count)], axis=1)
    bits = [1 << b for b in range(1, sections.bit_length() - 1)]
    joint = {0: column}
    for bit in bits:
        joint[bit] = exchanged(column, bit)
    values = {m: joint[m][0] for m in joint}
    outputs = {m: joint[m][1] for m in joint}
    single_value, single_output = {}, {}
    for mask in range(2, sections, 2):
        if mask in joint:
            continue
        high = 1 << (mask.bit_length() - 1)
        low = mask & -mask
        values[mask] = single_value[mask] = exchanged(values[mask ^ high], high)
    for mask in sorted(range(2, sections, 2), key=lambda m: bin(m).count("1")):
        if mask in joint:
            continue
        low = mask & -mask
        outputs[mask] = single_output[mask] = exchanged(outputs[mask ^ low], low)
    for part in (joint, single_value, single_output):
        for mask in list(part):
            part[mask ^ 1] = exchanged(part[mask], 1)
    return (joint, single_value, single_output)


def stack_kernel(layout, sizes, table_ref, tokens_ref, cotangent_ref, *refs):
    layers, old, sections, count, depth = sizes
    pieces = refs[: len(layout)]
    grads_ref, local_ref, value, output, streams, preacts, units, flowing, sems = refs[len(layout) :]
    myself = table_ref[layers + 2]
    mytp = table_ref[layers + 3]
    rows = depth // sections
    channels = value.shape[2]
    width = channels // count
    for place, (mask, matrices, first, number) in enumerate(layout):
        slab = jnp.bitwise_xor(myself, mask)
        row_at = pl.ds(pl.multiple_of(slab * rows, rows), rows)
        for index in range(number):
            for rotation in range(count):
                owner = lax.rem(mytp - rotation + count, count)
                lane_at = pl.ds(pl.multiple_of(owner * width, width), width)
                for order, matrix in enumerate(matrices):
                    target = (value, output)[matrix]
                    piece = pieces[place]
                    source = piece.at[order, rotation, index] if len(matrices) > 1 else piece.at[rotation, index]
                    pltpu.make_async_copy(
                        source, target.at[first + index, row_at, lane_at], sems.at[matrix, first + index]
                    ).start()
    streams[0] = tokens_ref[...]
    flowing[...] = cotangent_ref[...]
    grads_ref[...] = jnp.zeros_like(grads_ref)
    local_ref[...] = jnp.zeros_like(local_ref)

    def forward(j, carry):
        old_layer = table_ref[j]
        before = table_ref[jnp.maximum(j - 1, 0)]

        @pl.when((j == 0) | (before != old_layer))
        def _():
            for matrix, target in enumerate((value, output)):
                pltpu.make_async_copy(
                    target.at[old_layer], target.at[old_layer], sems.at[matrix, old_layer]
                ).wait()

        stream = streams[j].astype(jnp.float32)
        factor = lax.rsqrt(jnp.mean(stream * stream, axis=-1, keepdims=True) + epsilon)
        hidden = (stream * factor).astype(jnp.bfloat16)
        preact = jnp.dot(hidden, value[old_layer], preferred_element_type=jnp.float32)
        unit_values = (preact / (1.0 + jnp.exp(-preact))).astype(jnp.bfloat16)
        preacts[j] = preact
        units[j] = unit_values

        @pl.when(j < layers - 1)
        def _():
            mixing = lax.dot_general(
                unit_values, output[old_layer], (((1,), (1,)), ((), ())), preferred_element_type=jnp.float32
            )
            streams[j + 1] = (streams[j].astype(jnp.float32) + mixing).astype(jnp.bfloat16)

        return carry

    lax.fori_loop(0, layers, forward, 0)
    mine_at = pl.ds(pl.multiple_of(mytp * width, width), width)

    def backward(step, carry):
        j = layers - 1 - step
        old_layer = table_ref[j]
        grad_out = flowing[...]
        grad_units = jnp.dot(grad_out, output[old_layer], preferred_element_type=jnp.float32)
        preact = preacts[j]
        gate_value = 1.0 / (1.0 + jnp.exp(-preact))
        grad_inner = (grad_units * gate_value * (1.0 + preact * (1.0 - gate_value))).astype(jnp.bfloat16)
        preacts[j] = grad_inner.astype(jnp.float32)
        stream = streams[j].astype(jnp.float32)
        factor = lax.rsqrt(jnp.mean(stream * stream, axis=-1, keepdims=True) + epsilon)
        normed = stream * factor
        for which in range(2):

            @pl.when(table_ref[layers + which] == j)
            def _():
                inner = preacts[j, :, mine_at].astype(jnp.bfloat16)
                grads_ref[which, 0] = lax.dot_general(
                    normed.astype(jnp.bfloat16), inner, (((0,), (0,)), ((), ())), preferred_element_type=jnp.float32
                )
                grads_ref[which, 1] = lax.dot_general(
                    grad_out, units[j, :, mine_at], (((0,), (0,)), ((), ())), preferred_element_type=jnp.float32
                )
                if which == 0:
                    local_ref[0] = value[old_layer, :, mine_at]
                    local_ref[1] = output[old_layer, :, mine_at]

        @pl.when(j > 0)
        def _():
            grad_hidden = lax.dot_general(
                grad_inner, value[old_layer], (((1,), (1,)), ((), ())), preferred_element_type=jnp.float32
            )
            mean = jnp.mean(grad_hidden * normed, axis=-1, keepdims=True)
            flowing[...] = (
                flowing[...].astype(jnp.float32) + factor * (grad_hidden - normed * mean)
            ).astype(jnp.bfloat16)

        return carry

    lax.fori_loop(0, layers, backward, 0)


def replicated_body(
    tokens,
    cotangent,
    value_weight,
    output_weight,
    value_first,
    output_first,
    value_second,
    output_second,
    layer_map,
    old_section,
    new_section,
):
    sections, count = lax.axis_size("section"), lax.axis_size("tp")
    myself, mytp = lax.axis_index("section"), lax.axis_index("tp")
    layers, old = layer_map.shape[0], old_section.shape[0]
    depth, width = value_weight.shape[1:]
    rows = depth // sections
    has_layer, owned, source = layer_tables(layer_map, old_section, new_section, sections)

    my_tokens = token_share(tokens)
    weights = jnp.concatenate(
        [value_weight.reshape(sections, 1, rows, width), output_weight.reshape(sections, 1, rows, width)], axis=1
    )
    spread = lax.all_to_all(weights, "section", split_axis=0, concat_axis=0, tiled=True)
    chosen = jnp.stack([lax.dynamic_index_in_dim(spread, old_section[i], 0, False) for i in range(old)], axis=1)
    chunks = 2 if old % 2 == 0 else 1
    number = old // chunks
    layout, pieces = [], []
    for chunk in range(chunks):
        first = chunk * number
        joint, single_value, single_output = gathered_pieces(chosen[:, first : first + number])
        for part, matrices in ((joint, (0, 1)), (single_value, (0,)), (single_output, (1,))):
            for mask in part:
                layout.append((mask, matrices, first, number))
                pieces.append(part[mask])
    my_cotangent = token_share(cotangent)

    moments = jnp.stack(
        [m.astype(jnp.bfloat16).reshape(sections, rows, width) for m in (value_first, output_first, value_second, output_second)],
        axis=1,
    )
    moments = lax.all_to_all(moments, "section", split_axis=0, concat_axis=0, tiled=True)
    moments = jnp.stack([lax.dynamic_index_in_dim(moments, source[i], 0, False) for i in range(sections)])
    moments = lax.all_to_all(moments, "section", split_axis=0, concat_axis=0, tiled=True)
    moments = moments.transpose(1, 0, 2, 3).reshape(4, depth, width).astype(jnp.float32)
    holds = has_layer[myself].astype(jnp.float32)
    moments = moments * holds

    table = jnp.concatenate(
        [layer_map, jnp.stack([owned[myself], owned[jnp.bitwise_xor(myself, 1)], myself, mytp])]
    ).astype(jnp.int32)
    share = my_tokens.shape[0]
    channels = width * count
    any_space = pl.BlockSpec(memory_space=pl.ANY)
    vmem_space = pl.BlockSpec(memory_space=pltpu.VMEM)
    grads, local = pl.pallas_call(
        functools.partial(stack_kernel, tuple(layout), (layers, old, sections, count, depth)),
        in_specs=[pl.BlockSpec(memory_space=pltpu.SMEM), vmem_space, vmem_space] + [any_space] * len(pieces),
        out_specs=[vmem_space, vmem_space],
        out_shape=[
            jax.ShapeDtypeStruct((2, 2, depth, width), jnp.float32),
            jax.ShapeDtypeStruct((2, depth, width), jnp.bfloat16),
        ],
        scratch_shapes=[
            pltpu.VMEM((old, depth, channels), jnp.bfloat16),
            pltpu.VMEM((old, depth, channels), jnp.bfloat16),
            pltpu.VMEM((layers, share, depth), jnp.bfloat16),
            pltpu.VMEM((layers, share, channels), jnp.float32),
            pltpu.VMEM((layers, share, channels), jnp.bfloat16),
            pltpu.VMEM((share, depth), jnp.bfloat16),
            pltpu.SemaphoreType.DMA((2, old)),
        ],
        compiler_params=pltpu.CompilerParams(vmem_limit_bytes=vmem_budget),
        cost_estimate=pl.CostEstimate(
            flops=9 * layers * share * depth * channels, bytes_accessed=4 * old * depth * channels, transcendentals=0
        ),
        name="stack",
    )(table, my_tokens, my_cotangent, *pieces)
    gradient = grads[0] + exchanged(grads[1].astype(jnp.bfloat16), 1).astype(jnp.float32)
    value_new = adam_update(local[0], moments[0], moments[2], gradient[0])
    output_new = adam_update(local[1], moments[1], moments[3], gradient[1])
    return (value_new[0], output_new[0], value_new[1], output_new[1], value_new[2], output_new[2])


def chip_need(layers, old, share, depth, channels):
    weights = 4 * old * depth * channels
    kept = layers * share * (2 * depth + 6 * channels)
    return weights + kept + 14 * share * depth


def body(*arguments):
    tokens, value_weight, layer_map, old_section = arguments[0], arguments[2], arguments[8], arguments[9]
    sections, count = lax.axis_size("section"), lax.axis_size("tp")
    depth, width = value_weight.shape[1:]
    need = chip_need(
        layer_map.shape[0], old_section.shape[0], tokens.shape[0] * count // 2, depth, width * count
    )
    even = sections & (sections - 1) == 0 and sections > 1 and count % 2 == 0
    if even and depth % sections == 0 and need <= vmem_budget:
        return replicated_body(*arguments)
    return cascade_body(*arguments)


def solution(mesh):
    placed = (
        P("tp", None),
        P("tp", None),
        P("section", None, "tp"),
        P("section", None, "tp"),
        P("section", None, "tp"),
        P("section", None, "tp"),
        P("section", None, "tp"),
        P("section", None, "tp"),
        P(),
        P(),
        P(),
    )
    return jax.shard_map(
        body,
        mesh=mesh,
        in_specs=placed,
        out_specs=(
            P("section", None, "tp"),
            P("section", None, "tp"),
            P("section", None, "tp"),
            P("section", None, "tp"),
            P("section", None, "tp"),
            P("section", None, "tp"),
        ),
        check_vma=False,
    )
```
